32 devices in a mesh: section: 2 (over x), row: 4 (over y, core), col: 4 (over z).
Axes of the slice: x: 2, y: 2, z: 4, core: 2. Of those that a mesh axis runs over, the one named last changes fastest.
Arguments:
- inputs: bfloat16 [2, 1024, 2048], P(None, 'col', 'row'), may hold values from -6 to 6
- positions: int32 [2, 1024], P(None, 'col'), may hold values from 0 to 765, as said below
- cotangent: bfloat16 [2, 1024, 2048], P(None, 'col', 'row'), may hold values from -6 to 6
- norm_gains: float32 [2, 2, 2048], P('section'), may hold values from 0.5 to 1.5
- norm_biases: float32 [2, 2, 2048], P('section'), may hold values from -2 to 2
- qkv_weight: bfloat16 [2, 2048, 6144], P('section', 'col', 'row')
- qkv_bias: float32 [2, 6144], P('section', 'row'), may hold values from -3 to 3
- dense_weight: bfloat16 [2, 2048, 2048], P('section', 'row', 'col'), may hold values from -0.375 to 0.375
- dense_bias: float32 [2, 2048], P('section', 'row'), may hold values from -2 to 2
- fc1_weight: bfloat16 [2, 2048, 8192], P('section', 'col', 'row'), may hold values from -0.125 to 0.125
- fc1_bias: float32 [2, 8192], P('section', 'row'), may hold values from -3 to 3
- fc2_weight: bfloat16 [2, 8192, 2048], P('section', 'row', 'col'), may hold values from -0.0625 to 0.0625
- fc2_bias: float32 [2, 2048], P('section', 'row'), may hold values from -2 to 2
Outputs:
- section_outputs: bfloat16 [2, 2, 1024, 2048], P('section', None, 'col', 'row')
- input_grads: float32 [2, 2, 1024, 2048], P('section', None, 'col', 'row')
- qkv_weight_grad: float32 [2, 2048, 6144], P('section', 'col', 'row')
- qkv_bias_grad: float32 [2, 6144], P('section', 'row')
- dense_weight_grad: float32 [2, 2048, 2048], P('section', 'row', 'col')
- out_bias_grad: float32 [2, 2048], P('section', 'row')
- fc1_weight_grad: float32 [2, 2048, 8192], P('section', 'col', 'row')
- fc1_bias_grad: float32 [2, 8192], P('section', 'row')
- fc2_weight_grad: float32 [2, 8192, 2048], P('section', 'row', 'col')
- norm_gain_grad: float32 [2, 2, 2048], P('section')
- norm_bias_grad: float32 [2, 2, 2048], P('section')
The draws below stay inside these ranges and needn't reach their ends.
Inputs may be any that keep to these rules, and one draw needn't show every extreme that they name: Each sequence of 256 tokens starts at position 0, and positions rise by 1 to 3 from one token to the next; the first sequence of the first micro-batch rises by 3 at every token.
All inputs are finite; a program needn't handle non-finite values.
Results may differ from the reference program's by a relative error of at most 0.012.
Values may be sent and summed in bfloat16 or wider, within the bound.
A program may use at most 256 MiB of HBM per device.

```python
import math
import jax
import jax.numpy as jnp
from jax import lax

D = 2048
HEADS = 8
HEAD_DIM = 256
ROT = 64
FF = 8192
LEN = 256
MICRO = 2
SEQS = 4
TOKENS = 1024


def draw_positions(key, part):
    increments = jax.random.randint(key, (MICRO, SEQS, LEN), 1, 4)
    increments = increments.at[0, 0].set(3)
    rising = jnp.cumsum(increments, axis=-1) - increments[..., :1]
    return rising.reshape(MICRO, SEQS * LEN).astype(jnp.int32)


def draw_qkv_weight(key, part):
    base = jnp.clip(jax.random.normal(key, (2, D, HEADS, 3, HEAD_DIM), jnp.float32), -6.0, 6.0) * D ** (-0.5)
    return base.reshape(2, D, 3 * D).astype(jnp.bfloat16)


def steps_of(own_key, extent, shards, least, top_value):
    def one(dim, shards_of):
        draws = jax.random.uniform(jax.random.fold_in(jax.random.fold_in(own_key, 6), dim), (shards_of,), jnp.float32, least / len(shards), top_value / len(shards))
        return jnp.repeat(jnp.exp(draws), extent[dim] // shards_of).reshape((-1,) + (1,) * (len(extent) - dim - 1))

    level = one(*shards[0])
    for cut in shards[1:]:
        level = level * one(*cut)
    return level


def centred(own_key, shape, width, bound, split=(), dtype=jnp.bfloat16):
    values = jax.random.normal(own_key, shape, jnp.float32) * width
    if len(split) > 0:
        values = steps_of(own_key, shape, split, -0.22, 0.18) * values
    return jnp.clip(values, min=-bound, max=bound).astype(dtype)


def setup_inputs(seed: int = 0) -> dict:
    keys = jax.random.split(jax.random.key(seed), 14)
    inputs = centred(keys[0], (MICRO, TOKENS, D), 1.0, 6.0, ((1, 4), (2, 4)))
    positions = draw_positions(jax.random.fold_in(keys[13], 71), 0)
    cotangent = centred(keys[2], (MICRO, TOKENS, D), 1.0, 6.0, ((1, 4), (2, 4)))
    norm_gains = jnp.clip(1.0 + 0.1 * jax.random.normal(keys[3], (2, 2, D), jnp.float32), 0.5, 1.5)
    norm_biases = centred(keys[4], (2, 2, D), 0.3, 2.0, ((0, 2),), jnp.float32)
    qkv_weight = draw_qkv_weight(jax.random.fold_in(keys[13], 71), 0)
    qkv_bias = centred(keys[6], (2, 3 * D), 0.5, 3.0, ((0, 2), (1, 4)), jnp.float32)
    dense_weight = centred(keys[7], (2, D, D), (D // 8) ** -0.5, 0.375, ((0, 2), (1, 4), (2, 4)))
    dense_bias = centred(keys[8], (2, D), 0.3, 2.0, ((0, 2), (1, 4)), jnp.float32)
    fc1_weight = centred(keys[9], (2, D, FF), D ** -0.5, 0.125, ((0, 2), (1, 4), (2, 4)))
    fc1_bias = centred(keys[10], (2, FF), 0.5, 3.0, ((0, 2), (1, 4)), jnp.float32)
    fc2_weight = centred(keys[11], (2, FF, D), FF ** -0.5, 0.0625, ((0, 2), (1, 4), (2, 4)))
    fc2_bias = centred(keys[12], (2, D), 0.3, 2.0, ((0, 2), (1, 4)), jnp.float32)
    return dict(inputs=inputs, positions=positions, cotangent=cotangent, norm_gains=norm_gains, norm_biases=norm_biases, qkv_weight=qkv_weight, qkv_bias=qkv_bias, dense_weight=dense_weight, dense_bias=dense_bias, fc1_weight=fc1_weight, fc1_bias=fc1_bias, fc2_weight=fc2_weight, fc2_bias=fc2_bias)


NORM_EPS = 1e-05

def layer_norm(field_rows, gain, shift):
    center = field_rows - lax.optimization_barrier(jnp.mean(field_rows, axis=-1, keepdims=True))
    rstd_value = lax.rsqrt(lax.optimization_barrier(jnp.mean(center * center, axis=-1, keepdims=True)) + NORM_EPS)
    normed = center * rstd_value
    return (normed * gain + shift, normed, rstd_value)

def norm_back(grad_rows, normed, rstd_value, gain):
    scaled = grad_rows * gain
    return rstd_value * (scaled - lax.optimization_barrier(jnp.mean(scaled, axis=-1, keepdims=True)) - normed * lax.optimization_barrier(jnp.mean(scaled * normed, axis=-1, keepdims=True)))

def rotary_tables(place_ids, rotary_dims):
    half_dims = rotary_dims // 2
    powers = jnp.arange(half_dims).astype(jnp.float32) * (2.0 / rotary_dims)
    inverse = jnp.exp(-math.log(10000.0) * powers)
    angles = place_ids.astype(jnp.float32)[:, None] * inverse[None, :]
    return (jnp.cos(angles), jnp.sin(angles))

def rotate_pairs(vectors, cosines, sines, rotary_dims, direction):
    half_dims = rotary_dims // 2
    lower = vectors[..., :half_dims]
    upper = vectors[..., half_dims:rotary_dims]
    cos_part = cosines[:, None, :]
    sin_part = direction * sines[:, None, :]
    return jnp.concatenate([lower * cos_part - upper * sin_part, upper * cos_part + lower * sin_part, vectors[..., rotary_dims:]], axis=-1)

def gelu_parts(pre_act):
    cdf_value = 0.5 * (1.0 + lax.erf(pre_act * 0.5 ** 0.5))
    density = jnp.exp(-0.5 * pre_act * pre_act) * (2.0 * math.pi) ** (-0.5)
    return (pre_act * cdf_value, cdf_value + pre_act * density)

def round_low(array):
    return lax.optimization_barrier(array.astype(jnp.bfloat16))

def masked_scores(query_rows, key_rows):
    length = query_rows.shape[0]
    scores = jnp.einsum('qhd,khd->hqk', query_rows.astype(jnp.float32), key_rows.astype(jnp.float32)) * query_rows.shape[-1] ** (-0.5)
    allowed = jnp.arange(length)[:, None] >= jnp.arange(length)[None, :]
    return jnp.where(allowed, scores, -jnp.inf)

def seq_attend(packed):
    query_rows, key_rows, value_rows = packed
    scores = masked_scores(query_rows, key_rows)
    row_top = lax.optimization_barrier(jnp.max(scores, axis=-1, keepdims=True))
    logsum = row_top + jnp.log(lax.optimization_barrier(jnp.sum(jnp.exp(scores - row_top), axis=-1, keepdims=True)))
    probs = round_low(jnp.exp(scores - logsum))
    attended = jnp.einsum('hqk,khd->qhd', probs.astype(jnp.float32), value_rows.astype(jnp.float32))
    return (attended, logsum)

def seq_attend_back(packed):
    query_rows, key_rows, value_rows, attended, logsum, grad_rows = packed
    scores = masked_scores(query_rows, key_rows)
    probs = jnp.exp(scores - logsum)
    probs_low = round_low(probs).astype(jnp.float32)
    grad_wide = grad_rows.astype(jnp.float32)
    d_values = jnp.einsum('hqk,qhd->khd', probs_low, grad_wide)
    d_probs = jnp.einsum('qhd,khd->hqk', grad_wide, value_rows.astype(jnp.float32))
    row_dots = jnp.transpose(lax.optimization_barrier(jnp.sum(grad_wide * attended.astype(jnp.float32), axis=-1)))[:, :, None]
    d_scores = round_low(probs * (d_probs - row_dots) * query_rows.shape[-1] ** (-0.5)).astype(jnp.float32)
    d_query = jnp.einsum('hqk,khd->qhd', d_scores, key_rows.astype(jnp.float32))
    d_keys = jnp.einsum('hqk,qhd->khd', d_scores, query_rows.astype(jnp.float32))
    return (d_query, d_keys, d_values)

def layer_forward(layer_input, place_ids, layer_params):
    norm_gain, norm_shift, w_qkv, b_qkv, w_dense, b_dense, w_fc1, b_fc1, w_fc2, b_fc2 = layer_params
    field_rows = layer_input.astype(jnp.float32)
    first_low = layer_norm(field_rows, norm_gain[0], norm_shift[0])[0].astype(jnp.bfloat16)
    second_low = layer_norm(field_rows, norm_gain[1], norm_shift[1])[0].astype(jnp.bfloat16)
    token_count = layer_input.shape[0]
    mixed = (jnp.dot(first_low, w_qkv, preferred_element_type=jnp.float32) + b_qkv).reshape(token_count, HEADS, 3, HEAD_DIM)
    cosines, sines = rotary_tables(place_ids, ROT)
    query_rows = rotate_pairs(mixed[:, :, 0], cosines, sines, ROT, 1.0).astype(jnp.bfloat16)
    key_rows = rotate_pairs(mixed[:, :, 1], cosines, sines, ROT, 1.0).astype(jnp.bfloat16)
    value_rows = mixed[:, :, 2].astype(jnp.bfloat16)
    seq_shape = (token_count // LEN, LEN, HEADS, HEAD_DIM)
    attended, logsum = lax.map(seq_attend, (query_rows.reshape(seq_shape), key_rows.reshape(seq_shape), value_rows.reshape(seq_shape)))
    attn_out = attended.reshape(token_count, HEADS * HEAD_DIM).astype(jnp.bfloat16)
    pre_act = jnp.dot(second_low, w_fc1, preferred_element_type=jnp.float32) + b_fc1
    activation = gelu_parts(pre_act)[0].astype(jnp.bfloat16)
    branch_sum = jnp.dot(attn_out, w_dense, preferred_element_type=jnp.float32) + jnp.dot(activation, w_fc2, preferred_element_type=jnp.float32)
    layer_output = (field_rows + branch_sum + b_dense + b_fc2).astype(jnp.bfloat16)
    return (layer_output, (query_rows, key_rows, value_rows, attn_out, logsum, pre_act, activation))

def layer_backward(layer_input, place_ids, layer_params, saved_state, grad_out):
    norm_gain, norm_shift, w_qkv, b_qkv, w_dense, b_dense, w_fc1, b_fc1, w_fc2, b_fc2 = layer_params
    query_rows, key_rows, value_rows, attn_out, logsum, pre_act, activation = saved_state
    field_rows = layer_input.astype(jnp.float32)
    first_norm, first_hat, first_rstd = layer_norm(field_rows, norm_gain[0], norm_shift[0])
    second_norm, second_hat, second_rstd = layer_norm(field_rows, norm_gain[1], norm_shift[1])
    first_low = first_norm.astype(jnp.bfloat16)
    second_low = second_norm.astype(jnp.bfloat16)
    token_count = layer_input.shape[0]
    d_attn = jnp.dot(grad_out, w_dense.T, preferred_element_type=jnp.float32).astype(jnp.bfloat16)
    d_activ = jnp.dot(grad_out, w_fc2.T, preferred_element_type=jnp.float32)
    d_pre = d_activ * gelu_parts(pre_act)[1]
    d_pre_low = d_pre.astype(jnp.bfloat16)
    g_fc2 = jnp.dot(activation.T, grad_out, preferred_element_type=jnp.float32)
    g_dense = jnp.dot(attn_out.T, grad_out, preferred_element_type=jnp.float32)
    g_fc1 = jnp.dot(second_low.T, d_pre_low, preferred_element_type=jnp.float32)
    seq_shape = (token_count // LEN, LEN, HEADS, HEAD_DIM)
    d_query, d_keys, d_values = lax.map(seq_attend_back, (query_rows.reshape(seq_shape), key_rows.reshape(seq_shape), value_rows.reshape(seq_shape), attn_out.reshape(seq_shape), logsum, d_attn.reshape(seq_shape)))
    cosines, sines = rotary_tables(place_ids, ROT)
    head_shape = (token_count, HEADS, HEAD_DIM)
    d_query = rotate_pairs(d_query.reshape(head_shape), cosines, sines, ROT, -1.0)
    d_keys = rotate_pairs(d_keys.reshape(head_shape), cosines, sines, ROT, -1.0)
    d_mixed = jnp.stack([d_query, d_keys, d_values.reshape(head_shape)], axis=2).reshape(token_count, 3 * HEADS * HEAD_DIM)
    d_mixed_low = d_mixed.astype(jnp.bfloat16)
    g_qkv = jnp.dot(first_low.T, d_mixed_low, preferred_element_type=jnp.float32)
    back_first = jnp.dot(d_mixed_low, w_qkv.T, preferred_element_type=jnp.float32)
    back_second = jnp.dot(d_pre_low, w_fc1.T, preferred_element_type=jnp.float32)
    d_input = grad_out.astype(jnp.float32) + norm_back(back_first, first_hat, first_rstd, norm_gain[0]) + norm_back(back_second, second_hat, second_rstd, norm_gain[1])
    gain_terms = jnp.stack([lax.optimization_barrier(jnp.sum(back_first * first_hat, axis=0)), lax.optimization_barrier(jnp.sum(back_second * second_hat, axis=0))])
    shift_terms = jnp.stack([lax.optimization_barrier(jnp.sum(back_first, axis=0)), lax.optimization_barrier(jnp.sum(back_second, axis=0))])
    grads = (g_qkv, lax.optimization_barrier(jnp.sum(d_mixed, axis=0)), g_dense, lax.optimization_barrier(jnp.sum(grad_out.astype(jnp.float32), axis=0)), g_fc1, lax.optimization_barrier(jnp.sum(d_pre, axis=0)), g_fc2, gain_terms, shift_terms)
    return (d_input, grads)

def reference(inputs, positions, cotangent, norm_gains, norm_biases, qkv_weight, qkv_bias, dense_weight, dense_bias, fc1_weight, fc1_bias, fc2_weight, fc2_bias):
    section_params = []
    for section_index in range(2):
        section_params.append((norm_gains[section_index], norm_biases[section_index], qkv_weight[section_index], qkv_bias[section_index], dense_weight[section_index], dense_bias[section_index], fc1_weight[section_index], fc1_bias[section_index], fc2_weight[section_index], fc2_bias[section_index]))
    first_outputs, second_outputs, first_grads, second_grads = ([], [], [], [])
    totals = [None, None]
    for micro_index in range(MICRO):
        place_ids = positions[micro_index]
        first_out, first_saved = layer_forward(inputs[micro_index], place_ids, section_params[0])
        second_out, second_saved = layer_forward(first_out, place_ids, section_params[1])
        second_input_grad, second_terms = layer_backward(first_out, place_ids, section_params[1], second_saved, cotangent[micro_index])
        first_input_grad, first_terms = layer_backward(inputs[micro_index], place_ids, section_params[0], first_saved, second_input_grad.astype(jnp.bfloat16))
        first_outputs.append(first_out)
        second_outputs.append(second_out)
        first_grads.append(first_input_grad)
        second_grads.append(second_input_grad)
        for section_index, terms in ((0, first_terms), (1, second_terms)):
            if totals[section_index] is None:
                totals[section_index] = terms
            else:
                totals[section_index] = tuple((running + update for running, update in zip(totals[section_index], terms)))
    section_outputs = jnp.stack([jnp.stack(first_outputs), jnp.stack(second_outputs)])
    input_grads = jnp.stack([jnp.stack(first_grads), jnp.stack(second_grads)])
    stacked = [jnp.stack([totals[0][member], totals[1][member]]) for member in range(9)]
    return (section_outputs, input_grads, stacked[0], stacked[1], stacked[2], stacked[3], stacked[4], stacked[5], stacked[6], stacked[7], stacked[8])
```

```python
import functools
import math

import jax
import jax.numpy as jnp
from jax import lax
from jax.experimental import pallas as pl
from jax.experimental.pallas import tpu as pltpu
from jax.sharding import PartitionSpec as P

HEAD_DIM = 256
ROT = 64
LEN = 256
NORM_EPS = 1e-05
BF16 = jnp.bfloat16
F32 = jnp.float32


def dot32(left, right):
    return jnp.dot(left, right, preferred_element_type=F32)


def dot_nt(left, right):
    return lax.dot_general(left, right, (((1,), (1,)), ((), ())), preferred_element_type=F32)


def dot_tn(left, right):
    return lax.dot_general(left, right, (((0,), (0,)), ((), ())), preferred_element_type=F32)


def rotary_tables(place_ids, rotary_dims):
    half_dims = rotary_dims // 2
    powers = jnp.arange(half_dims).astype(F32) * (2.0 / rotary_dims)
    inverse = jnp.exp(-math.log(10000.0) * powers)
    angles = place_ids.astype(F32)[:, None] * inverse[None, :]
    return (jnp.cos(angles), jnp.sin(angles))


def rotate_pairs(vectors, cosines, sines, direction):
    half_dims = ROT // 2
    lower = vectors[..., :half_dims]
    upper = vectors[..., half_dims:ROT]
    cos_part = cosines[:, None, :]
    sin_part = direction * sines[:, None, :]
    return jnp.concatenate(
        [
            lower * cos_part - upper * sin_part,
            upper * cos_part + lower * sin_part,
            vectors[..., ROT:],
        ],
        axis=-1,
    )


def gelu_parts(pre_act):
    cdf_value = 0.5 * (1.0 + lax.erf(pre_act * 0.5**0.5))
    density = jnp.exp(-0.5 * pre_act * pre_act) * (2.0 * math.pi) ** (-0.5)
    return (pre_act * cdf_value, cdf_value + pre_act * density)


def causal_scores(query_seq, key_seq):
    length = query_seq.shape[1]
    scores = jnp.einsum(
        "sqhd,skhd->shqk", query_seq, key_seq, preferred_element_type=F32
    ) * query_seq.shape[-1] ** (-0.5)
    allowed = jnp.arange(length)[:, None] >= jnp.arange(length)[None, :]
    return jnp.where(allowed, scores, -jnp.inf)


def half_of(array, axis, index, count):
    width = array.shape[axis] // count
    return lax.dynamic_slice_in_dim(array, index * width, width, axis)


def section_params(mine, other, section, layer):
    return jnp.where(section == layer, mine, other)


def spread_weight(shard, axis, section, sections, layer):
    own = half_of(shard, axis, section, sections)
    sent = half_of(shard, axis, 1 - section, sections)
    received = lax.ppermute(sent, "section", [(layer, 1 - layer)])
    return jnp.where(section == layer, own, received)


MESH = pl.DeviceIdType.MESH


def flipped(index, bit):
    return index + bit - 2 * bit * ((index // bit) % 2)


def greet(partners):
    barrier = pltpu.get_barrier_semaphore()
    for partner in partners:
        pl.semaphore_signal(barrier, inc=1, device_id=partner, device_id_type=MESH)
    pl.semaphore_wait(barrier, len(partners))


def peer_of(cols):
    return {"col": lax.rem(lax.axis_index("col") + cols // 2, cols)}


def row_bits(row_count):
    bits, bit = [], row_count // 2
    while bit >= 1:
        bits.append(bit)
        bit //= 2
    return bits


def gather_kernel(row_count, cols, chunks, block_ref, out_ref, send_sems, recv_sems, local_sem):
    me = lax.axis_index("row")
    rows, width = block_ref.shape
    bits = row_bits(row_count)
    peer = peer_of(cols)
    greet([peer] + [{"row": flipped(me, bit)} for bit in bits])
    step = rows // chunks
    started = []

    def columns(index):
        return pl.ds(pl.multiple_of(index * width, width), width)

    def send(source, target, partner):
        number = len(started)
        copy = pltpu.make_async_remote_copy(
            src_ref=source,
            dst_ref=target,
            send_sem=send_sems.at[number],
            recv_sem=recv_sems.at[number],
            device_id=partner,
            device_id_type=MESH,
        )
        copy.start()
        started.append(copy)
        return copy

    def spread(source_of, target_of, ready):
        ready()
        held = [(me, None)]
        for bit in bits:
            fresh = []
            for index, copy in held:
                if copy is not None:
                    copy.wait_recv()
                sent = send(source_of(index, copy), target_of(index), {"row": flipped(me, bit)})
                fresh.append((flipped(index, bit), sent))
            held = [(index, None) for index, _ in held] + fresh
        return held

    peer_copies = []
    for chunk in range(chunks):
        part = pl.ds(chunk * step, step)
        peer_copies.append(send(block_ref.at[part], out_ref.at[1, part, columns(me)], peer))
    local = pltpu.make_async_copy(block_ref, out_ref.at[0, :, columns(me)], local_sem)
    local.start()
    groups = []
    groups.append((0, pl.ds(0, rows), None))
    for chunk in range(chunks):
        groups.append((1, pl.ds(chunk * step, step), peer_copies[chunk]))
    held = []
    waited = set()
    state = []
    for place, part, arrival in groups:
        state.append([(me, arrival)])
    for bit in bits:
        for number, (place, part, _) in enumerate(groups):
            fresh = []
            for index, copy in state[number]:
                if copy is not None and id(copy) not in waited:
                    copy.wait_recv()
                    waited.add(id(copy))
                own = place == 0 and index is me
                source = block_ref if own else out_ref.at[place, part, columns(index)]
                sent = send(source, out_ref.at[place, part, columns(index)], {"row": flipped(me, bit)})
                fresh.append((flipped(index, bit), sent))
            state[number] = state[number] + fresh
    for copy in started:
        if id(copy) not in waited:
            copy.wait_recv()
        copy.wait_send()
    local.wait()


def gather_rows(block):
    row_count, cols = lax.axis_size("row"), lax.axis_size("col")
    rows, width = block.shape
    chunks = 2
    copies = chunks + (chunks + 1) * (row_count - 1)
    return pl.pallas_call(
        functools.partial(gather_kernel, row_count, cols, chunks),
        out_shape=jax.ShapeDtypeStruct((2, rows, row_count * width), block.dtype),
        in_specs=[pl.BlockSpec(memory_space=pltpu.VMEM)],
        out_specs=pl.BlockSpec(memory_space=pl.ANY),
        scratch_shapes=[
            pltpu.SemaphoreType.DMA((copies,)),
            pltpu.SemaphoreType.DMA((copies,)),
            pltpu.SemaphoreType.DMA,
        ],
        compiler_params=pltpu.CompilerParams(collective_id=1, has_side_effects=True),
        name="gather_rows",
    )(block)


def reduce_kernel(row_count, cols, chunks, with_peer, *refs):
    count = len(with_peer)
    ins = sum(2 if both else 1 for both in with_peer)
    in_refs, refs = refs[:ins], refs[ins:]
    out_refs, refs = refs[:count], refs[count:]
    first_buf, first_send, pair_buf, pair_send, last_buf, last_send, send_sems, recv_sems = refs
    me = lax.axis_index("row")
    section = lax.axis_index("section")
    rows, features = in_refs[0].shape
    width = features // row_count
    bits = row_bits(row_count)[::-1]
    peer = peer_of(cols)
    other = {"section": 1 - section}
    greet([peer, other] + [{"row": flipped(me, bit)} for bit in bits])
    step = rows // chunks
    started = []

    def columns(index):
        return pl.ds(pl.multiple_of(index * width, width), width)

    def send(source, target, partner):
        number = len(started)
        copy = pltpu.make_async_remote_copy(
            src_ref=source,
            dst_ref=target,
            send_sem=send_sems.at[number],
            recv_sem=recv_sems.at[number],
            device_id=partner,
            device_id_type=MESH,
        )
        copy.start()
        started.append(copy)
        return copy

    own_slots, items, slot = [], [], 0
    for output, both in enumerate(with_peer):
        own_slots.append(slot)
        if both:
            for chunk in range(chunks):
                items.append((slot + 1, chunk, output, True))
        slot += 2 if both else 1
    for output, both in enumerate(with_peer):
        for chunk in range(chunks):
            items.append((own_slots[output], chunk, output, False))

    def subsets(low_bits):
        masks = [[]]
        for bit in low_bits:
            masks = masks + [mask + [bit] for mask in masks]
        return masks

    def moved(index, mask):
        for bit in mask:
            index = flipped(index, bit)
        return index

    pending = []
    for slot, chunk, output, is_peer in items:
        part = pl.ds(chunk * step, step)
        partner = flipped(me, bits[0])
        copies = []
        for number, mask in enumerate(subsets(bits[1:])):
            copies.append(
                send(
                    in_refs[slot].at[part, columns(moved(partner, mask))],
                    first_buf.at[slot, number, part],
                    {"row": partner},
                )
            )
        pending.append(copies)
    sums = []
    for (slot, chunk, output, is_peer), copies in zip(items, pending):
        part = pl.ds(chunk * step, step)
        held = []
        for number, mask in enumerate(subsets(bits[1:])):
            copies[number].wait_recv()
            held.append(
                (
                    mask,
                    in_refs[slot][part, columns(moved(me, mask))].astype(F32)
                    + first_buf[slot, number, part].astype(F32),
                )
            )
        sums.append(held)
        if len(bits) > 1:
            kept = []
            sent = []
            for mask, value in held:
                if bits[1] in mask:
                    first_send[slot, part] = value.astype(BF16)
                    sent.append(
                        send(first_send.at[slot, part], pair_buf.at[slot, part], {"row": flipped(me, bits[1])})
                    )
                else:
                    pair_send[slot, part] = value
            pending[items.index((slot, chunk, output, is_peer))] = sent
    peers = {}
    lasts = {}
    for (slot, chunk, output, is_peer), copies in zip(items, pending):
        part = pl.ds(chunk * step, step)
        copies[0].wait_recv()
        value = pair_send[slot, part] + pair_buf[slot, part].astype(F32)
        if is_peer:
            last_send[slot, part] = value.astype(BF16)
            peers[(output, chunk)] = (
                slot,
                send(last_send.at[slot, part], last_buf.at[slot, part], peer),
            )
        else:
            if (output, chunk) in peers:
                peer_slot, copy = peers[(output, chunk)]
                copy.wait_recv()
                value = value + last_buf[peer_slot, part].astype(F32)
            last_send[slot, part] = value.astype(BF16)
            lasts[(output, chunk)] = (
                slot,
                send(last_send.at[slot, part], last_buf.at[slot, part], other),
            )
    for (output, chunk), (slot, copy) in lasts.items():
        part = pl.ds(chunk * step, step)
        copy.wait_recv()
        out_refs[output][part] = last_send[slot, part].astype(F32) + last_buf[slot, part].astype(F32)
    for copy in started:
        copy.wait_send()


def reduce_rows(pairs, collective_id):
    row_count, cols = lax.axis_size("row"), lax.axis_size("col")
    assert row_count == 4
    rows, features = pairs[0][0].shape
    width = features // row_count
    with_peer = tuple(peer is not None for _, peer in pairs)
    operands = [member for pair in pairs for member in pair if member is not None]
    slots = len(operands)
    chunks = 4
    copies = slots * chunks * (row_count // 2 + 1 + 1)
    return pl.pallas_call(
        functools.partial(reduce_kernel, row_count, cols, chunks, with_peer),
        out_shape=[jax.ShapeDtypeStruct((rows, width), F32) for _ in pairs],
        in_specs=[pl.BlockSpec(memory_space=pltpu.VMEM)] * slots,
        out_specs=[pl.BlockSpec(memory_space=pltpu.VMEM)] * len(pairs),
        scratch_shapes=[
            pltpu.VMEM((slots, row_count // 2, rows, width), BF16),
            pltpu.VMEM((slots, rows, width), BF16),
            pltpu.VMEM((slots, rows, width), BF16),
            pltpu.VMEM((slots, rows, width), F32),
            pltpu.VMEM((slots, rows, width), BF16),
            pltpu.VMEM((slots, rows, width), BF16),
            pltpu.SemaphoreType.DMA((copies,)),
            pltpu.SemaphoreType.DMA((copies,)),
        ],
        compiler_params=pltpu.CompilerParams(collective_id=collective_id, has_side_effects=True),
        name="reduce_rows",
    )(*operands)


def stats_kernel(row_count, in_ref, out_ref, buf, send, send_sems, recv_sems):
    me = lax.axis_index("row")
    bits = row_bits(row_count)
    greet([{"row": flipped(me, bit)} for bit in bits])
    value = in_ref[...]
    for number, bit in enumerate(bits):
        send[number] = value
        copy = pltpu.make_async_remote_copy(
            src_ref=send.at[number],
            dst_ref=buf.at[number],
            send_sem=send_sems.at[number],
            recv_sem=recv_sems.at[number],
            device_id={"row": flipped(me, bit)},
            device_id_type=MESH,
        )
        copy.start()
        copy.wait()
        value = value + buf[number]
    out_ref[...] = value


def row_sum(stats):
    row_count = lax.axis_size("row")
    stages = len(row_bits(row_count))
    return pl.pallas_call(
        functools.partial(stats_kernel, row_count),
        out_shape=jax.ShapeDtypeStruct(stats.shape, F32),
        in_specs=[pl.BlockSpec(memory_space=pltpu.VMEM)],
        out_specs=pl.BlockSpec(memory_space=pltpu.VMEM),
        scratch_shapes=[
            pltpu.VMEM((stages,) + stats.shape, F32),
            pltpu.VMEM((stages,) + stats.shape, F32),
            pltpu.SemaphoreType.DMA((stages,)),
            pltpu.SemaphoreType.DMA((stages,)),
        ],
        compiler_params=pltpu.CompilerParams(collective_id=4, has_side_effects=True),
        name="row_sum",
    )(stats)


def layer_forward(entry, params, weights, tables):
    gains, shifts, b_qkv, b_fc1, b_out = params
    w_qkv, w_fc1, w_dense, w_fc2 = weights
    cosines, sines = tables
    rows = entry.shape[0]
    field = gather_rows(entry).reshape(2 * rows, -1).astype(F32)
    center = field - jnp.mean(field, axis=-1, keepdims=True)
    rstd = lax.rsqrt(jnp.mean(center * center, axis=-1, keepdims=True) + NORM_EPS)
    normed = center * rstd
    first_low = (normed[:rows] * gains[0] + shifts[0]).astype(BF16)
    second_low = (normed * gains[1] + shifts[1]).astype(BF16)
    heads = w_qkv.shape[1] // (3 * HEAD_DIM)
    mixed = (dot32(first_low, w_qkv) + b_qkv).reshape(rows, heads, 3, HEAD_DIM)
    query = rotate_pairs(mixed[:, :, 0], cosines, sines, 1.0).astype(BF16)
    keys = rotate_pairs(mixed[:, :, 1], cosines, sines, 1.0).astype(BF16)
    values = mixed[:, :, 2].astype(BF16)
    seq = (rows // LEN, LEN, heads, HEAD_DIM)
    scores = causal_scores(query.reshape(seq), keys.reshape(seq))
    top = jnp.max(scores, axis=-1, keepdims=True)
    logsum = top + jnp.log(jnp.sum(jnp.exp(scores - top), axis=-1, keepdims=True))
    probs = jnp.exp(scores - logsum).astype(BF16)
    attended = jnp.einsum("shqk,skhd->sqhd", probs, values.reshape(seq), preferred_element_type=F32)
    attn_out = attended.reshape(rows, heads * HEAD_DIM).astype(BF16)
    pre_act = dot32(second_low, w_fc1) + b_fc1
    activation = gelu_parts(pre_act)[0].astype(BF16)
    own = (dot32(attn_out, w_dense) + dot32(activation[:rows], w_fc2)).astype(BF16)
    peers = dot32(activation[rows:], w_fc2).astype(BF16)
    (summed,) = reduce_rows([(own, peers)], 2)
    output = (entry.astype(F32) + summed + b_out).astype(BF16)
    return output, (center[:rows], rstd[:rows], first_low, second_low, query, keys, values, attn_out, logsum, pre_act, activation)


def layer_backward(grad, wide_grad, saved, params, weights, tables):
    gains = params[0]
    w_qkv, w_fc1, w_dense, w_fc2 = weights
    cosines, sines = tables
    center, rstd, first_low, second_low, query, keys, values, attn_out, logsum, pre_act, activation = saved
    rows, width = grad.shape
    wide_own = wide_grad[0]
    wide_grad = wide_grad.reshape(2 * rows, -1)
    g_fc2 = dot_tn(activation, wide_grad).astype(BF16)
    g_dense = dot_tn(attn_out, wide_own).astype(BF16)
    d_pre = dot_nt(wide_grad, w_fc2) * gelu_parts(pre_act)[1]
    d_pre_low = d_pre.astype(BF16)
    g_fc1 = dot_tn(second_low, d_pre_low).astype(BF16)
    d_attn = dot_nt(wide_own, w_dense).astype(BF16)
    heads = w_qkv.shape[1] // (3 * HEAD_DIM)
    seq = (rows // LEN, LEN, heads, HEAD_DIM)
    head_shape = (rows, heads, HEAD_DIM)
    query_seq, key_seq = query.reshape(seq), keys.reshape(seq)
    grad_seq = d_attn.reshape(seq)
    probs = jnp.exp(causal_scores(query_seq, key_seq) - logsum)
    d_values = jnp.einsum("shqk,sqhd->skhd", probs.astype(BF16), grad_seq, preferred_element_type=F32)
    d_probs = jnp.einsum("sqhd,skhd->shqk", grad_seq, values.reshape(seq), preferred_element_type=F32)
    row_dots = jnp.einsum("sqhd,sqhd->shq", grad_seq, attn_out.reshape(seq), preferred_element_type=F32)[..., None]
    d_scores = (probs * (d_probs - row_dots) * HEAD_DIM ** (-0.5)).astype(BF16)
    d_query = jnp.einsum("shqk,skhd->sqhd", d_scores, key_seq, preferred_element_type=F32).reshape(head_shape)
    d_keys = jnp.einsum("shqk,sqhd->skhd", d_scores, query_seq, preferred_element_type=F32).reshape(head_shape)
    d_query = rotate_pairs(d_query, cosines, sines, -1.0)
    d_keys = rotate_pairs(d_keys, cosines, sines, -1.0)
    d_mixed = jnp.stack([d_query, d_keys, d_values.reshape(head_shape)], axis=2).reshape(rows, 3 * heads * HEAD_DIM)
    d_mixed_low = d_mixed.astype(BF16)
    g_qkv = dot_tn(first_low, d_mixed_low).astype(BF16)
    back_first = dot_nt(d_mixed_low, w_qkv).astype(BF16)
    back_second = dot_nt(d_pre_low, w_fc1).astype(BF16)
    totals = reduce_rows([(back_first, None), (back_second[:rows], back_second[rows:])], 3)
    row_index = lax.axis_index("row")
    row_count = lax.axis_size("row")
    my_normed = half_of(center, 1, row_index, row_count) * rstd
    my_gains = half_of(gains, 1, row_index, row_count)
    sums = []
    for total, my_gain in zip(totals, my_gains):
        scaled = total * my_gain
        sums.append(jnp.sum(scaled, axis=-1))
        sums.append(jnp.sum(scaled * my_normed, axis=-1))
    stats = row_sum(jnp.stack(sums + sums)) / (row_count * width)
    d_input = grad.astype(F32)
    gain_terms, shift_terms = [], []
    for index, total in enumerate(totals):
        d_input = d_input + rstd * (
            total * my_gains[index] - stats[2 * index][:, None] - my_normed * stats[2 * index + 1][:, None]
        )
        gain_terms.append(jnp.sum(total * my_normed, axis=0))
        shift_terms.append(jnp.sum(total, axis=0))
    small = (
        jnp.stack(gain_terms + shift_terms),
        jnp.sum(d_mixed, axis=0),
        jnp.sum(d_pre, axis=0),
        jnp.sum(grad.astype(F32), axis=0),
    )
    return d_input, (g_qkv, g_fc1, g_dense, g_fc2), small


AXES = (1, 1, 0, 0)


def halves_of(cols):
    group = cols // 2
    return [list(range(group)), list(range(group, cols))]


def peer_pairs(cols):
    return [(index, (index + cols // 2) % cols) for index in range(cols)]


def gather_hidden(part, axis, half, cols):
    other = 1 - axis
    own = half_of(part, axis, half, 2)
    received = lax.ppermute(half_of(part, axis, 1 - half, 2), "col", peer_pairs(cols))
    stacked = jnp.stack([jnp.where(half == 0, own, received), jnp.where(half == 0, received, own)])
    wide = lax.all_gather(stacked, "col", axis=0, axis_index_groups=halves_of(cols))
    if other == 0:
        return wide.transpose(1, 0, 2, 3).reshape(cols * own.shape[0], own.shape[1])
    return wide.transpose(2, 1, 0, 3).reshape(own.shape[0], cols * own.shape[1])


def scatter_hidden(grad, axis, half, cols):
    group = cols // 2
    if axis == 1:
        stacked = grad.reshape(2, group, grad.shape[0] // cols, grad.shape[1]).transpose(1, 0, 2, 3)
    else:
        stacked = grad.reshape(grad.shape[0], 2, group, grad.shape[1] // cols).transpose(2, 1, 0, 3)
    mine = lax.psum_scatter(stacked, "col", scatter_dimension=0, axis_index_groups=halves_of(cols))
    own = jnp.where(half == 0, mine[0], mine[1])
    received = lax.ppermute(jnp.where(half == 0, mine[1], mine[0]), "col", peer_pairs(cols))
    return jnp.concatenate([jnp.where(half == 0, own, received), jnp.where(half == 0, received, own)], axis=axis)


def scatter_grads(grads, half, cols):
    g_qkv, g_fc1, g_dense, g_fc2 = grads
    return (
        lax.psum_scatter(g_qkv, "col", scatter_dimension=0, tiled=True),
        scatter_hidden(g_fc1, 1, half, cols),
        lax.psum_scatter(g_dense, "col", scatter_dimension=1, tiled=True),
        scatter_hidden(g_fc2, 0, half, cols),
    )


def local(
    inputs,
    positions,
    cotangent,
    norm_gains,
    norm_biases,
    qkv_weight,
    qkv_bias,
    dense_weight,
    dense_bias,
    fc1_weight,
    fc1_bias,
    fc2_weight,
    fc2_bias,
):
    sections = lax.axis_size("section")
    section = lax.axis_index("section")
    cols = lax.axis_size("col")
    half = lax.axis_index("col") // (cols // 2)
    micro, tokens, width = inputs.shape
    rows = micro * tokens
    shards = (qkv_weight[0], fc1_weight[0], dense_weight[0], fc2_weight[0])

    own = (norm_gains[0], norm_biases[0], qkv_bias[0], fc1_bias[0], dense_bias[0] + fc2_bias[0])
    packed = jnp.concatenate([member.reshape(-1) for member in own])
    theirs = lax.ppermute(packed, "section", [(0, 1), (1, 0)])
    layer_params = []
    for layer in range(sections):
        flat = section_params(packed, theirs, section, layer)
        members, start = [], 0
        for member in own:
            members.append(flat[start : start + member.size].reshape(member.shape))
            start += member.size
        gains, shifts, b_qkv, b_fc1, b_out = members
        layer_params.append(
            (gains, shifts, half_of(b_qkv, 0, section, sections), half_of(b_fc1, 0, 2 * section + half, 2 * sections), b_out)
        )

    tables = rotary_tables(positions.reshape(rows), ROT)
    weights = []
    for layer in range(sections):
        parts = [spread_weight(shard, axis, section, sections, layer) for shard, axis in zip(shards, AXES)]
        weights.append(
            (
                lax.all_gather(parts[0], "col", axis=0, tiled=True),
                gather_hidden(parts[1], 1, half, cols),
                lax.all_gather(parts[2], "col", axis=1, tiled=True),
                gather_hidden(parts[3], 0, half, cols),
            )
        )

    entry = inputs.reshape(rows, width)
    outputs, saves = [], []
    for layer in range(sections):
        entry, saved = layer_forward(entry, layer_params[layer], weights[layer], tables)
        outputs.append(entry)
        saves.append(saved)

    grad = cotangent.reshape(rows, width)
    input_grads, part_grads, returned, smalls = [None] * sections, [None] * sections, [None] * sections, [None] * sections
    for layer in reversed(range(sections)):
        wide_grad = gather_rows(grad)
        d_input, grads, small = layer_backward(
            grad, wide_grad, saves[layer], layer_params[layer], weights[layer], tables
        )
        input_grads[layer] = d_input
        grad = d_input.astype(BF16)
        part_grads[layer] = scatter_grads(grads, half, cols)
        returned[layer] = tuple(
            lax.ppermute(member, "section", [(1 - layer, layer)]) for member in part_grads[layer]
        )
        hidden_term = jnp.where(jnp.arange(2)[:, None] == half, small[2][None], 0.0).reshape(-1)
        smalls[layer] = small[:2] + (hidden_term,) + small[3:]

    first = section == 0

    def pick(values):
        return jnp.where(first, values[0], values[1])

    weight_grads = []
    for index, axis in enumerate(AXES):
        mine = pick([part_grads[layer][index] for layer in range(sections)]).astype(F32)
        other = pick([returned[layer][index] for layer in range(sections)]).astype(F32)
        weight_grads.append(
            jnp.concatenate([jnp.where(first, mine, other), jnp.where(first, other, mine)], axis=axis)[None]
        )

    norm_terms = pick([smalls[layer][0] for layer in range(sections)])
    out_term = pick([smalls[layer][3] for layer in range(sections)])
    bias_mine = pick([jnp.concatenate([smalls[layer][1], smalls[layer][2]]) for layer in range(sections)])
    bias_sent = pick([jnp.concatenate([smalls[layer][1], smalls[layer][2]]) for layer in reversed(range(sections))])
    bias_other = lax.ppermute(bias_sent, "section", [(0, 1), (1, 0)])
    summed = lax.psum(jnp.concatenate([norm_terms.reshape(-1), out_term, bias_mine, bias_other]), "col")
    count = norm_terms.size
    norm_sums = lax.all_gather(summed[:count].reshape(4, width), "row", axis=1, tiled=True)
    out_bias_grad = summed[count : count + width]
    qkv_size = smalls[0][1].size
    fc1_size = smalls[0][2].size
    mine = summed[count + width : count + width + qkv_size + fc1_size]
    other = summed[count + width + qkv_size + fc1_size :]
    lower = jnp.where(first, mine, other)
    upper = jnp.where(first, other, mine)
    qkv_bias_grad = jnp.concatenate([lower[:qkv_size], upper[:qkv_size]])
    fc1_bias_grad = jnp.concatenate([lower[qkv_size:], upper[qkv_size:]])
    shape = (1, micro, tokens, width)
    return (
        pick(outputs).reshape(shape),
        pick(input_grads).reshape(shape),
        weight_grads[0],
        qkv_bias_grad[None],
        weight_grads[2],
        out_bias_grad[None],
        weight_grads[1],
        fc1_bias_grad[None],
        weight_grads[3],
        norm_sums[None, :2],
        norm_sums[None, 2:],
    )


def solution(mesh):
    in_specs = (
        P(None, "col", "row"),
        P(None, "col"),
        P(None, "col", "row"),
        P("section", None, None),
        P("section", None, None),
        P("section", "col", "row"),
        P("section", "row"),
        P("section", "row", "col"),
        P("section", "row"),
        P("section", "col", "row"),
        P("section", "row"),
        P("section", "row", "col"),
        P("section", "row"),
    )
    out_specs = (
        P("section", None, "col", "row"),
        P("section", None, "col", "row"),
        P("section", "col", "row"),
        P("section", "row"),
        P("section", "row", "col"),
        P("section", "row"),
        P("section", "col", "row"),
        P("section", "row"),
        P("section", "row", "col"),
        P("section", None, None),
        P("section", None, None),
    )
    return jax.shard_map(local, mesh=mesh, in_specs=in_specs, out_specs=out_specs, check_vma=False)
```
